32 devices in a mesh: img: 4 (over y, core), txt: 8 (over z, x).
Axes of the slice: x: 2, y: 2, z: 4, core: 2. Of those that a mesh axis runs over, the one named last changes fastest.
Arguments:
- queries: bfloat16 [1, 5120, 8192], P(None, 'txt', 'img'), may hold values from -128 to 128
- visual_keys: bfloat16 [1, 512, 8192], P(None, 'img'), may hold values from -5 to 5
- visual_values: bfloat16 [1, 512, 8192], P(None, 'img'), may hold values from -6 to 6
- out_grad: bfloat16 [1, 5120, 8192], P(None, 'txt', 'img'), may hold values from -6 to 6
- gate_value: float32 [1, 64], P(None, 'img'), may hold values from -1.5 to 1.5
- image_order: int32 [1, 8], replicated, may hold values from 0 to 7, as said below
- image_seen: int32 [5120], P('txt'), may hold values from 1 to 8
Outputs:
- query_grad: bfloat16 [1, 5120, 8192], P(None, 'txt', 'img')
- key_grad: float32 [1, 512, 8192], P(None, 'txt', 'img')
- value_grad: float32 [1, 512, 8192], P(None, 'txt', 'img')
The draws below stay inside these ranges and needn't reach their ends.
Inputs may be any that keep to these rules, and one draw needn't show every extreme that they name: `image_order`: each row names every image of 0 to 7 once.
All inputs are finite; a program needn't handle non-finite values.
Results may differ from the reference program's by a relative error of at most 0.0058.
Values may be sent and summed in bfloat16 or wider, within the bound.
A program may use at most 128 MiB of HBM per device.

```python
import math
import jax
import jax.numpy as jnp
from jax import lax

D = 8192
H = 64
HD = 128
LAT = 64
IMAGES = 8
LAYERS = 1
TOK_DEV = 640
TOKENS = 5120
KEYS = 512


def order_table(key):
    row_list = [jax.random.permutation(jax.random.fold_in(key, 100 + layer_index), IMAGES) for layer_index in range(LAYERS)]
    return jnp.stack(row_list).astype(jnp.int32)


def key_table(key):
    normal_table = jnp.clip(jax.random.normal(jax.random.fold_in(key, 7), (LAYERS, KEYS, D), jnp.float32), -5.0, 5.0)
    return normal_table


def draw_image_order(key, part):
    return order_table(key)


def draw_visual_keys(key, part):
    return key_table(key).astype(jnp.bfloat16)


def draw_queries(key, part):
    normal_table = jnp.clip(jax.random.normal(jax.random.fold_in(key, 9), (LAYERS, TOKENS, D), jnp.float32), -5.0, 5.0)
    return normal_table.astype(jnp.bfloat16)


def set_ends(drawn, stream_key, low, largest):
    spot = [jax.random.randint(jax.random.fold_in(stream_key, axis), (), 0, length) for axis, length in enumerate(drawn.shape)]
    widest = drawn.shape.index(max(drawn.shape))
    neighbour = spot[:widest] + [(spot[widest] + 1) % drawn.shape[widest]] + spot[widest + 1:]
    return drawn.at[tuple(spot)].set(low).at[tuple(neighbour)].set(largest)


def shard_levels(rng, dims, split, least, largest):
    def one(dim, shards_of):
        heights = jax.random.uniform(jax.random.fold_in(jax.random.fold_in(rng, 6), dim), (shards_of,), jnp.float32, least / len(split), largest / len(split))
        return jnp.repeat(jnp.exp(heights), dims[dim] // shards_of).reshape((-1,) + (1,) * (len(dims) - dim - 1))

    level = one(*split[0])
    for cut in split[1:]:
        level = level * one(*cut)
    return level


def scatter_about(stream_key, extent, width, most, shards=(), dtype=jnp.bfloat16):
    gain = shard_levels(stream_key, extent, shards, -0.22, 0.18) if shards else 1.0
    entries = jax.random.normal(stream_key, extent, jnp.float32) * width * gain
    return jnp.minimum(jnp.maximum(entries, -most), most).astype(dtype)


def setup_inputs(seed: int = 0) -> dict:
    streams_of = jax.random.split(jax.random.key(seed), 8)
    queries = draw_queries(jax.random.fold_in(streams_of[7], 71), 0)
    visual_keys = draw_visual_keys(jax.random.fold_in(streams_of[7], 71), 0)
    visual_values = scatter_about(streams_of[2], (LAYERS, KEYS, D), 1.0, 6.0, ((1, 4),))
    out_grad = scatter_about(streams_of[3], (LAYERS, TOKENS, D), 1.0, 6.0, ((1, 8), (2, 4)))
    gate_value = jnp.clip(jax.random.uniform(streams_of[4], (LAYERS, H), jnp.float32, -1.5, 1.5) * shard_levels(streams_of[4], (LAYERS, H), ((1, 4),), -0.4, 0.0), -1.5, 1.5)
    image_order = draw_image_order(jax.random.fold_in(streams_of[7], 71), 0)
    image_seen = set_ends(jax.random.randint(streams_of[6], (TOKENS,), 1, IMAGES + 1), jax.random.fold_in(streams_of[6], 1), 1, IMAGES).astype(jnp.int32)
    return dict(queries=queries, visual_keys=visual_keys, visual_values=visual_values, out_grad=out_grad, gate_value=gate_value, image_order=image_order, image_seen=image_seen)


def rounded(array):
    return lax.optimization_barrier(array.astype(jnp.bfloat16)).astype(jnp.float32)

def reference(queries, visual_keys, visual_values, out_grad, gate_value, image_order, image_seen):
    score_scale = 1.0 / math.sqrt(HD)
    block_count = TOKENS // TOK_DEV
    query_list = []
    key_list = []
    value_list = []
    for layer_index in range(LAYERS):
        key_image = jnp.broadcast_to(image_order[layer_index][:, None], (IMAGES, LAT)).reshape(KEYS)
        key_heads = visual_keys[layer_index].astype(jnp.float32).reshape(KEYS, H, HD)
        value_heads = visual_values[layer_index].astype(jnp.float32).reshape(KEYS, H, HD)
        factor = jnp.tanh(gate_value[layer_index])

        def block_step(totals, pieces):
            query_block, grad_block, seen_block = pieces
            query_heads = query_block.astype(jnp.float32).reshape(TOK_DEV, H, HD)
            gated_grad = rounded(grad_block.astype(jnp.float32).reshape(TOK_DEV, H, HD) * factor[None, :, None])
            allowed = key_image[None, :] < seen_block[:, None]
            scores = jnp.einsum('thd,khd->htk', query_heads, key_heads) * score_scale
            masked = jnp.where(allowed[None], scores, -1e+30)
            row_max = lax.optimization_barrier(jnp.max(masked, axis=2, keepdims=True))
            exponent = jnp.where(allowed[None], jnp.exp(masked - row_max), 0.0)
            weights = exponent / lax.optimization_barrier(jnp.sum(exponent, axis=2, keepdims=True))
            weight_half = rounded(weights)
            attended = jnp.einsum('htk,khd->thd', weight_half, value_heads)
            row_delta = lax.optimization_barrier(jnp.sum(gated_grad * attended, axis=2))
            weight_grad = jnp.einsum('thd,khd->htk', gated_grad, value_heads)
            score_half = rounded(weights * (weight_grad - jnp.transpose(row_delta)[:, :, None]))
            query_part = (jnp.einsum('htk,khd->thd', score_half, key_heads) * score_scale).astype(jnp.bfloat16)
            key_part = jnp.einsum('htk,thd->khd', score_half, query_heads) * score_scale
            value_part = jnp.einsum('htk,thd->khd', weight_half, gated_grad)
            new_totals = (totals[0] + key_part.reshape(KEYS, D), totals[1] + value_part.reshape(KEYS, D))
            return (new_totals, query_part.reshape(TOK_DEV, D))
        inputs = (queries[layer_index].reshape(block_count, TOK_DEV, D), out_grad[layer_index].reshape(block_count, TOK_DEV, D), image_seen.reshape(block_count, TOK_DEV))
        empty_sum = jnp.zeros((KEYS, D), jnp.float32)
        sums, query_parts = lax.scan(block_step, (empty_sum, empty_sum), inputs)
        query_list.append(query_parts.reshape(TOKENS, D))
        key_list.append(sums[0])
        value_list.append(sums[1])
    return (jnp.stack(query_list), jnp.stack(key_list), jnp.stack(value_list))
```

```python
import functools
import math

import jax
import jax.numpy as jnp
from jax import lax
from jax.experimental import pallas as pl
from jax.experimental.pallas import tpu as pltpu
from jax.sharding import PartitionSpec as P

NT = (((1,), (1,)), ((), ()))
TN = (((0,), (0,)), ((), ()))
NN = (((1,), (0,)), ((), ()))


def matmul(left, right, dims):
    return lax.dot_general(left, right, dims, preferred_element_type=jnp.float32)


def head_grads(query, gated, key, value, bias):
    rows, tokens = key.shape[0], query.shape[0]
    images = bias.shape[0]
    scale = 1.0 / math.sqrt(query.shape[1])
    scores = matmul(key, query, NT) * (scale * math.log2(math.e))
    masked = (scores.reshape(images, rows // images, tokens) + bias[:, None, :]).reshape(rows, tokens)
    exponent = jnp.exp2(masked - jnp.max(masked, axis=0, keepdims=True))
    weights = exponent * (1.0 / jnp.sum(exponent, axis=0, keepdims=True))
    weight_half = weights.astype(jnp.bfloat16)
    weight_grad = matmul(value, gated, NT)
    delta = jnp.sum(weight_half.astype(jnp.float32) * weight_grad, axis=0, keepdims=True)
    score_half = (weights * (weight_grad - delta)).astype(jnp.bfloat16)
    query_grad = (matmul(key, score_half, TN) * scale).T
    key_grad = matmul(score_half, query, NN) * scale
    value_grad = matmul(weight_half, gated, NN)
    return query_grad, key_grad, value_grad


def kernel(images_n, sides, order_ref, factor_ref, seen_ref, query_ref, grad_ref, key_ref, value_ref,
           out_ref, key_out, value_out,
           bias, latents, part, pair_out, pair_in, far_out, far_in,
           latent_send, latent_recv, pair_send, pair_recv, far_send, far_recv):
    head = pl.program_id(0)
    heads = pl.num_programs(0)
    width = query_ref.shape[1]
    owned = key_ref.shape[0]
    me = lax.axis_index("img")
    place = lax.axis_index("txt")
    mine = place // 2
    side = place % 2
    other = 1 - side
    partner = {"txt": mine * 2 + other}

    def latent_copy(source, index, slot, off):
        owner = (me + off) % images_n
        column = pl.multiple_of((owner * heads + index) * width, width)
        view = source.at[:, pl.ds(column, width)]
        target = latents.at[index, slot, pl.ds(pl.multiple_of(me * owned, owned), owned), :]
        if off == 0:
            return pltpu.make_async_copy(view, target, latent_recv.at[index])
        return pltpu.make_async_remote_copy(
            src_ref=view, dst_ref=target, send_sem=latent_send.at[index],
            recv_sem=latent_recv.at[index], device_id={"img": owner},
            device_id_type=pl.DeviceIdType.MESH)

    def pair_copy(index):
        return pltpu.make_async_remote_copy(
            src_ref=pair_out.at[index], dst_ref=pair_in.at[index],
            send_sem=pair_send.at[index], recv_sem=pair_recv.at[index],
            device_id=partner, device_id_type=pl.DeviceIdType.MESH)

    def far_copy(index, off):
        there = (mine + off) % sides
        return pltpu.make_async_remote_copy(
            src_ref=far_out.at[index, off - 1], dst_ref=far_in.at[index, off - 1],
            send_sem=far_send.at[index], recv_sem=far_recv.at[index],
            device_id={"txt": there * 2 + side}, device_id_type=pl.DeviceIdType.MESH)

    def drain(ref, sem):
        pltpu.make_async_copy(ref, ref, sem).wait()

    def columns(index):
        return pl.ds(pl.multiple_of(index * width, width), width)

    @pl.when(head == 0)
    def _():
        barrier = pltpu.get_barrier_semaphore()
        peers = [{"img": (me + off) % images_n} for off in range(1, images_n)] + [partner]
        peers += [{"txt": ((mine + off) % sides) * 2 + side} for off in range(1, sides)]
        for peer in peers:
            pl.semaphore_signal(barrier, inc=1, device_id=peer, device_id_type=pl.DeviceIdType.MESH)
        pl.semaphore_wait(barrier, len(peers))

        def send(index, carry):
            for off in list(range(1, images_n)) + [0]:
                latent_copy(key_ref, index, 0, off).start()
                latent_copy(value_ref, index, 1, off).start()
            return carry

        lax.fori_loop(0, heads, send, 0)
        for i in range(order_ref.shape[0]):
            bias[pl.ds(i, 1), :] = jnp.where(seen_ref[...] > order_ref[i], 0.0, -1e30)

    def relay(index):
        pair_copy(index).wait_recv()
        slot = index % 2
        for off in range(1, sides):
            there = (mine + off) % sides
            for kind in range(2):
                far_out[index, off - 1, kind] = (
                    part[slot, kind, there * 2 + side]
                    + pair_in[index, kind, there].astype(jnp.float32)
                ).astype(jnp.bfloat16)
        for off in range(1, sides):
            far_copy(index, off).start()
        for kind, out in enumerate((key_out, value_out)):
            out[:, columns(index)] = (
                part[slot, kind, mine * 2 + side] + pair_in[index, kind, mine].astype(jnp.float32)
            )

    def finish(index):
        drain(far_in.at[index], far_recv.at[index])
        for kind, out in enumerate((key_out, value_out)):
            total = out[:, columns(index)]
            for off in range(1, sides):
                total = total + far_in[index, off - 1, kind].astype(jnp.float32)
            out[:, columns(index)] = total

    drain(latents.at[head], latent_recv.at[head])
    gated = (grad_ref[...].astype(jnp.float32) * factor_ref[head]).astype(jnp.bfloat16)
    query_grad, key_grad, value_grad = head_grads(
        query_ref[...], gated, latents[head, 0], latents[head, 1], bias[...]
    )
    out_ref[...] = query_grad.astype(out_ref.dtype)
    now = head % 2
    shape = part.shape[2:]
    part[now, 0] = key_grad.reshape(shape)
    part[now, 1] = value_grad.reshape(shape)
    for kind in range(2):
        for there in range(sides):
            pair_out[head, kind, there] = part[now, kind, there * 2 + other].astype(jnp.bfloat16)
    pair_copy(head).start()

    @pl.when(head >= 1)
    def _():
        relay(head - 1)

    @pl.when(head >= 2)
    def _():
        finish(head - 2)

    @pl.when(head == heads - 1)
    def _():
        relay(heads - 1)
        finish(heads - 2)
        finish(heads - 1)

        def settle(index, carry):
            drain(latents.at[index, :, pl.ds(0, owned * (images_n - 1)), :], latent_send.at[index])
            pair_copy(index).wait_send()
            drain(far_out.at[index], far_send.at[index])
            return carry

        lax.fori_loop(0, heads, settle, 0)


def attention(images_n, texts_n, order, factor, seen, query, grad, key, value):
    tokens, width = query.shape
    heads = factor.shape[0]
    head_width = width // heads
    owned = key.shape[0]
    rows = owned * images_n
    sides = texts_n // 2
    share = rows // texts_n
    smem = pl.BlockSpec(memory_space=pltpu.SMEM)
    hbm = pl.BlockSpec(memory_space=pl.ANY)
    column = pl.BlockSpec((tokens, head_width), lambda h: (0, h))
    fixed = pl.BlockSpec((share, width), lambda h: (0, 0))
    half = jnp.bfloat16
    dma = pltpu.SemaphoreType.DMA((heads,))
    return pl.pallas_call(
        functools.partial(kernel, images_n, sides),
        grid=(heads,),
        in_specs=[smem, smem, pl.BlockSpec((1, tokens), lambda h: (0, 0)), column, column, hbm, hbm],
        out_specs=[column, fixed, fixed],
        out_shape=[jax.ShapeDtypeStruct((tokens, width), half)]
        + [jax.ShapeDtypeStruct((share, width), jnp.float32)] * 2,
        scratch_shapes=[
            pltpu.VMEM((order.shape[0], tokens), jnp.float32),
            pltpu.VMEM((heads, 2, rows, head_width), half),
            pltpu.VMEM((2, 2, texts_n, share, head_width), jnp.float32),
            pltpu.VMEM((heads, 2, sides, share, head_width), half),
            pltpu.VMEM((heads, 2, sides, share, head_width), half),
            pltpu.VMEM((heads, sides - 1, 2, share, head_width), half),
            pltpu.VMEM((heads, sides - 1, 2, share, head_width), half),
            dma, dma, dma, dma, dma, dma,
        ],
        compiler_params=pltpu.CompilerParams(
            vmem_limit_bytes=56 * 1024 * 1024, collective_id=0, has_side_effects=True
        ),
    )(order, factor, seen, query, grad, key, value)


def shards(images_n, texts_n, queries, visual_keys, visual_values, out_grad, gate_value, image_order, image_seen):
    factor = jnp.tanh(gate_value[0])
    query_grad, key_share, value_share = attention(
        images_n, texts_n, image_order[0], factor, image_seen[None, :],
        queries[0], out_grad[0], visual_keys[0], visual_values[0]
    )
    return (query_grad[None], key_share[None], value_share[None])


def solution(mesh):
    placed = (
        P(None, "txt", "img"),
        P(None, "img", None),
        P(None, "img", None),
        P(None, "txt", "img"),
        P(None, "img"),
        P(),
        P("txt"),
    )
    return jax.shard_map(
        functools.partial(shards, mesh.shape["img"], mesh.shape["txt"]),
        mesh=mesh,
        in_specs=placed,
        out_specs=(P(None, "txt", "img"), P(None, "txt", "img"), P(None, "txt", "img")),
        check_vma=False,
    )
```

```python
import functools
import math

import jax
import jax.numpy as jnp
from jax import lax
from jax.experimental import pallas as pl
from jax.experimental.pallas import tpu as pltpu
from jax.sharding import PartitionSpec as P

NT = (((1,), (1,)), ((), ()))
TN = (((0,), (0,)), ((), ()))
NN = (((1,), (0,)), ((), ()))


def matmul(left, right, dims):
    return lax.dot_general(left, right, dims, preferred_element_type=jnp.float32)


def head_grads(query, gated, key, value, bias):
    rows, tokens = key.shape[0], query.shape[0]
    images = bias.shape[0]
    scale = 1.0 / math.sqrt(query.shape[1])
    scores = matmul(key, query, NT) * (scale * math.log2(math.e))
    masked = (scores.reshape(images, rows // images, tokens) + bias[:, None, :]).reshape(rows, tokens)
    exponent = jnp.exp2(masked - jnp.max(masked, axis=0, keepdims=True))
    weights = exponent * (1.0 / jnp.sum(exponent, axis=0, keepdims=True))
    weight_half = weights.astype(jnp.bfloat16)
    weight_grad = matmul(value, gated, NT)
    delta = jnp.sum(weight_half.astype(jnp.float32) * weight_grad, axis=0, keepdims=True)
    score_half = (weights * (weight_grad - delta)).astype(jnp.bfloat16)
    query_grad = (matmul(key, score_half, TN) * scale).T
    key_grad = matmul(score_half, query, NN) * scale
    value_grad = matmul(weight_half, gated, NN)
    return query_grad, key_grad, value_grad


def kernel(images_n, sides, order_ref, gate_ref, seen_ref, query_ref, grad_ref, key_ref, value_ref,
           out_ref, key_out, value_out,
           bias, latents, part, pair_out, pair_in, far_out, far_in,
           latent_send, latent_recv, pair_send, pair_recv, far_send, far_recv):
    head = pl.program_id(0)
    heads = pl.num_programs(0)
    width = query_ref.shape[1]
    owned = key_ref.shape[0]
    me = lax.axis_index("img")
    place = lax.axis_index("txt")
    mine = place // 2
    side = place % 2
    other = 1 - side
    partner = {"txt": mine * 2 + other}

    def latent_copy(source, index, slot, off):
        owner = (me + off) % images_n
        column = pl.multiple_of((owner * heads + index) * width, width)
        view = source.at[:, pl.ds(column, width)]
        target = latents.at[index, slot, pl.ds(pl.multiple_of(me * owned, owned), owned), :]
        if off == 0:
            return pltpu.make_async_copy(view, target, latent_recv.at[index])
        return pltpu.make_async_remote_copy(
            src_ref=view, dst_ref=target, send_sem=latent_send.at[index],
            recv_sem=latent_recv.at[index], device_id={"img": owner},
            device_id_type=pl.DeviceIdType.MESH)

    def pair_copy(index):
        return pltpu.make_async_remote_copy(
            src_ref=pair_out.at[index], dst_ref=pair_in.at[index],
            send_sem=pair_send.at[index], recv_sem=pair_recv.at[index],
            device_id=partner, device_id_type=pl.DeviceIdType.MESH)

    def far_copy(index, off):
        there = (mine + off) % sides
        return pltpu.make_async_remote_copy(
            src_ref=far_out.at[index, off - 1], dst_ref=far_in.at[index, off - 1],
            send_sem=far_send.at[index], recv_sem=far_recv.at[index],
            device_id={"txt": there * 2 + side}, device_id_type=pl.DeviceIdType.MESH)

    def drain(ref, sem):
        pltpu.make_async_copy(ref, ref, sem).wait()

    def columns(index):
        return pl.ds(pl.multiple_of(index * width, width), width)

    @pl.when(head == 0)
    def _():
        barrier = pltpu.get_barrier_semaphore()
        peers = [{"img": (me + off) % images_n} for off in range(1, images_n)] + [partner]
        peers += [{"txt": ((mine + off) % sides) * 2 + side} for off in range(1, sides)]
        for peer in peers:
            pl.semaphore_signal(barrier, inc=1, device_id=peer, device_id_type=pl.DeviceIdType.MESH)
        pl.semaphore_wait(barrier, len(peers))

        def send(index, carry):
            for off in list(range(1, images_n)) + [0]:
                latent_copy(key_ref, index, 0, off).start()
                latent_copy(value_ref, index, 1, off).start()
            return carry

        lax.fori_loop(0, heads, send, 0)
        seen = seen_ref[...].reshape(1, bias.shape[1])
        for i in range(order_ref.shape[1]):
            bias[pl.ds(i, 1), :] = jnp.where(seen > order_ref[0, i], 0.0, -1e30)

    def relay(index):
        pair_copy(index).wait_recv()
        slot = index % 2
        for off in range(1, sides):
            there = (mine + off) % sides
            for kind in range(2):
                far_out[index, off - 1, kind] = (
                    part[slot, kind, there * 2 + side]
                    + pair_in[index, kind, there].astype(jnp.float32)
                ).astype(jnp.bfloat16)
        for off in range(1, sides):
            far_copy(index, off).start()
        for kind, out in enumerate((key_out, value_out)):
            out[:, columns(index)] = (
                part[slot, kind, mine * 2 + side] + pair_in[index, kind, mine].astype(jnp.float32)
            )

    def finish(index):
        drain(far_in.at[index], far_recv.at[index])
        for kind, out in enumerate((key_out, value_out)):
            total = out[:, columns(index)]
            for off in range(1, sides):
                total = total + far_in[index, off - 1, kind].astype(jnp.float32)
            out[:, columns(index)] = total

    drain(latents.at[head], latent_recv.at[head])
    lane = lax.broadcasted_iota(jnp.int32, gate_ref.shape, 1)
    gate = jnp.sum(jnp.where(lane == head, gate_ref[...], 0.0), axis=1, keepdims=True)
    gated = (grad_ref[...].astype(jnp.float32) * jnp.tanh(gate)).astype(jnp.bfloat16)
    query_grad, key_grad, value_grad = head_grads(
        query_ref[...], gated, latents[head, 0], latents[head, 1], bias[...]
    )
    out_ref[...] = query_grad.astype(out_ref.dtype)
    now = head % 2
    shape = part.shape[2:]
    part[now, 0] = key_grad.reshape(shape)
    part[now, 1] = value_grad.reshape(shape)
    for kind in range(2):
        for there in range(sides):
            pair_out[head, kind, there] = part[now, kind, there * 2 + other].astype(jnp.bfloat16)
    pair_copy(head).start()

    @pl.when(head >= 1)
    def _():
        relay(head - 1)

    @pl.when(head >= 2)
    def _():
        finish(head - 2)

    @pl.when(head == heads - 1)
    def _():
        relay(heads - 1)
        finish(heads - 2)
        finish(heads - 1)

        def settle(index, carry):
            drain(latents.at[index, :, pl.ds(0, owned * (images_n - 1)), :], latent_send.at[index])
            pair_copy(index).wait_send()
            drain(far_out.at[index], far_send.at[index])
            return carry

        lax.fori_loop(0, heads, settle, 0)


def attention(images_n, texts_n, order, gate, seen, query, grad, key, value):
    tokens, width = query.shape
    heads = gate.shape[1]
    head_width = width // heads
    owned = key.shape[0]
    rows = owned * images_n
    sides = texts_n // 2
    share = rows // texts_n
    smem = pl.BlockSpec(memory_space=pltpu.SMEM)
    hbm = pl.BlockSpec(memory_space=pl.ANY)
    column = pl.BlockSpec((tokens, head_width), lambda h: (0, h))
    fixed = pl.BlockSpec((share, width), lambda h: (0, 0))
    half = jnp.bfloat16
    dma = pltpu.SemaphoreType.DMA((heads,))
    return pl.pallas_call(
        functools.partial(kernel, images_n, sides),
        grid=(heads,),
        in_specs=[smem, pl.BlockSpec((1, heads), lambda h: (0, 0)),
                  pl.BlockSpec((tokens,), lambda h: (0,)), column, column, hbm, hbm],
        out_specs=[column, fixed, fixed],
        out_shape=[jax.ShapeDtypeStruct((tokens, width), half)]
        + [jax.ShapeDtypeStruct((share, width), jnp.float32)] * 2,
        scratch_shapes=[
            pltpu.VMEM((order.shape[1], tokens), jnp.float32),
            pltpu.VMEM((heads, 2, rows, head_width), half),
            pltpu.VMEM((2, 2, texts_n, share, head_width), jnp.float32),
            pltpu.VMEM((heads, 2, sides, share, head_width), half),
            pltpu.VMEM((heads, 2, sides, share, head_width), half),
            pltpu.VMEM((heads, sides - 1, 2, share, head_width), half),
            pltpu.VMEM((heads, sides - 1, 2, share, head_width), half),
            dma, dma, dma, dma, dma, dma,
        ],
        compiler_params=pltpu.CompilerParams(
            vmem_limit_bytes=56 * 1024 * 1024, collective_id=0, has_side_effects=True
        ),
    )(order, gate, seen, query, grad, key, value)


def shards(images_n, texts_n, queries, visual_keys, visual_values, out_grad, gate_value, image_order, image_seen):
    query_grad, key_share, value_share = attention(
        images_n, texts_n, image_order, gate_value, image_seen,
        queries[0], out_grad[0], visual_keys[0], visual_values[0]
    )
    return (query_grad[None], key_share[None], value_share[None])


def solution(mesh):
    placed = (
        P(None, "txt", "img"),
        P(None, "img", None),
        P(None, "img", None),
        P(None, "txt", "img"),
        P(None, "img"),
        P(),
        P("txt"),
    )
    return jax.shard_map(
        functools.partial(shards, mesh.shape["img"], mesh.shape["txt"]),
        mesh=mesh,
        in_specs=placed,
        out_specs=(P(None, "txt", "img"), P(None, "txt", "img"), P(None, "txt", "img")),
        check_vma=False,
    )
```
